8 devices in a mesh: dp: 2 (over z, y), tp: 4 (over x, core).
Axes of the slice: x: 2, y: 2, z: 1, core: 2. Of those that a mesh axis runs over, the one named last changes fastest.
Arguments:
- x_in: bfloat16 [256, 6656], P('dp', 'tp'), parts along dimension 0
- w_cross: bfloat16 [3, 6656, 6656], P(None, None, 'tp')
- b_cross: float32 [3, 6656], P(None, 'tp')
Outputs:
- output: bfloat16 [256, 6656], P('dp', 'tp'), parts along dimension 0
There are 2 independent parts. The reference program is written for one: setup_inputs(seed, part) draws one part's arguments, and reference() takes and returns one part's arrays. A program takes and returns all parts, laid end to end along the dimension named above; an argument that names none is the same for every part.
All inputs are finite; a program needn't handle non-finite values.
Results may differ from the reference program's by a relative error of at most 0.00176.
Values are sent between devices in bfloat16 or wider.
A program may use at most 1 GiB of HBM per device.

```python
import jax
import jax.numpy as jnp
from jax import lax

BATCH = 128
FIELDS = 26
EMB = 256
LAYERS = 3
D = FIELDS * EMB


def setup_inputs(seed: int = 0, part: int = 0) -> dict:
    base_key = jax.random.key(seed)
    key_x = jax.random.fold_in(jax.random.fold_in(base_key, 1), part)
    key_w = jax.random.fold_in(base_key, 2)
    key_b = jax.random.fold_in(base_key, 3)
    x_in = jax.random.normal(key_x, (BATCH, D), jnp.float32).astype(jnp.bfloat16)
    w_cross = (jax.random.normal(key_w, (LAYERS, D, D), jnp.float32) * (D ** -0.5)).astype(jnp.bfloat16)
    b_cross = 0.5 * jax.random.normal(key_b, (LAYERS, D), jnp.float32)
    return {"x_in": x_in, "w_cross": w_cross, "b_cross": b_cross}


def reference(x_in, w_cross, b_cross):
    x_first = x_in.astype(jnp.float32)

    def cross_layer(x_cur, layer_params):
        w_layer, b_layer = layer_params
        projected = jnp.dot(x_cur, w_layer, preferred_element_type=jnp.float32)
        x_next = (x_first * (projected + b_layer) + x_cur.astype(jnp.float32)).astype(jnp.bfloat16)
        return x_next, None

    x_out, _ = lax.scan(cross_layer, x_in, (w_cross, b_cross))
    return x_out
```

```python
import functools

import jax
import jax.numpy as jnp
from jax import lax
from jax.experimental import pallas as pl
from jax.experimental.pallas import tpu as pltpu
from jax.sharding import PartitionSpec as P

MESH = pl.DeviceIdType.MESH
LAYERS, D, COLS, ROWS = 3, 6656, 1664, 128
HALF = ROWS // 2
TILE = 128
NT = COLS // TILE
OWN, MATE, FAR, FARMATE = range(4)
CHUNKS = ((0, 4), (4, 8), (8, 12), (12, 13))
NC = len(CHUNKS)


def tiles(role, chunk):
    return [(role, t) for t in range(*CHUNKS[chunk])]


SEGMENTS = [
    [(OWN, t) for t in range(NT)] + [(MATE, t) for t in range(NT)],
    tiles(FAR, 0),
    tiles(FAR, 1) + tiles(FARMATE, 0),
    tiles(FAR, 2) + tiles(FARMATE, 1),
    tiles(FARMATE, 2),
    tiles(FAR, 3) + tiles(FARMATE, 3),
]
SEQ = [t for s in SEGMENTS for t in s]
BLOCKS = [(SEQ[2 * i], SEQ[2 * i + 1]) for i in range(len(SEQ) // 2)]
NB = len(BLOCKS)
SEG_BLOCKS = []
_b = 0
for _s in SEGMENTS:
    SEG_BLOCKS.append(list(range(_b, _b + len(_s) // 2)))
    _b += len(_s) // 2
SLOTS = 65
NTILES = [(n, min(256, COLS - n)) for n in range(0, COLS, 256)]


def kernel(x_hbm, w_hbm, b_hbm, out_hbm, xb, wb, acc, bias, stage, w_sem, x_sem, b_sem, o_sem,
           far_send, far_recv, fwd_send, fwd_recv, mate_send, mate_recv):
    me = lax.axis_index("tp")
    mate = me + 1 - 2 * lax.rem(me, 2)
    far = lax.rem(me + 2, 4)
    farmate = lax.rem(mate + 2, 4)
    owners = (me, mate, far, farmate)

    def w_copies(layer, block, start):
        slot = lax.rem(layer * NB + block, SLOTS)
        (r0, t0), (r1, t1) = BLOCKS[block]
        if not start:
            pltpu.make_async_copy(w_hbm.at[0, pl.ds(0, 2 * TILE)], wb.at[slot], w_sem.at[slot]).wait()
        elif r0 == r1:
            row = pl.multiple_of(owners[r0] * COLS + t0 * TILE, TILE)
            pltpu.make_async_copy(w_hbm.at[layer, pl.ds(row, 2 * TILE)], wb.at[slot], w_sem.at[slot]).start()
        else:
            for i, (r, t) in enumerate(((r0, t0), (r1, t1))):
                row = pl.multiple_of(owners[r] * COLS + t * TILE, TILE)
                pltpu.make_async_copy(
                    w_hbm.at[layer, pl.ds(row, TILE)], wb.at[slot, pl.ds(i * TILE, TILE)], w_sem.at[slot]
                ).start()

    def far_copy(p, c):
        t0, t1 = CHUNKS[c]
        return pltpu.make_async_remote_copy(
            xb.at[p, pl.ds(OWN * NT + t0, t1 - t0)], xb.at[p, pl.ds(FAR * NT + t0, t1 - t0)],
            far_send.at[p, c], far_recv.at[p, c], device_id={"tp": far}, device_id_type=MESH)

    def fwd_copy(p, c):
        t0, t1 = CHUNKS[c]
        return pltpu.make_async_remote_copy(
            xb.at[p, pl.ds(FAR * NT + t0, t1 - t0)], xb.at[p, pl.ds(FARMATE * NT + t0, t1 - t0)],
            fwd_send.at[p, c], fwd_recv.at[p, c], device_id={"tp": mate}, device_id_type=MESH)

    def mate_copy(p):
        return pltpu.make_async_remote_copy(
            xb.at[p, pl.ds(OWN * NT, NT)], xb.at[p, pl.ds(MATE * NT, NT)],
            mate_send.at[p], mate_recv.at[p], device_id={"tp": mate}, device_id_type=MESH)

    for h in range(2):
        for t in range(NT):
            pltpu.make_async_copy(
                x_hbm.at[pl.ds(h * HALF, HALF), pl.ds(t * TILE, TILE)], xb.at[h, OWN * NT + t], x_sem.at[h]
            ).start()
    barrier = pltpu.get_barrier_semaphore()
    for other in (mate, far):
        pl.semaphore_signal(barrier, inc=1, device_id={"tp": other}, device_id_type=MESH)
    pltpu.make_async_copy(b_hbm, bias, b_sem).start()
    pl.semaphore_wait(barrier, 2)
    for h in range(2):
        pltpu.make_async_copy(xb.at[h, pl.ds(0, NT)], xb.at[h, pl.ds(0, NT)], x_sem.at[h]).wait()
        for c in range(NC):
            far_copy(h, c).start()
        mate_copy(h).start()
    for layer in range(LAYERS):
        for block in range(NB):
            if layer * NB + block < SLOTS:
                w_copies(layer, block, True)
    pltpu.make_async_copy(b_hbm, bias, b_sem).wait()

    def x_block(p, block):
        (r0, t0), (r1, t1) = BLOCKS[block]
        return jnp.concatenate([xb[p, r0 * NT + t0], xb[p, r1 * NT + t1]], axis=1)

    def dots(layer, p, blocks, n, width):
        total = None
        for block in blocks:
            slot = lax.rem(layer * NB + block, SLOTS)
            term = jnp.dot(x_block(p, block), wb[slot, :, pl.ds(n, width)], preferred_element_type=jnp.float32)
            total = term if total is None else total + term
        return total

    def phase(layer, h):
        p = 2 * layer + h

        def segment(s):
            if h == 0:
                for block in SEG_BLOCKS[s]:
                    w_copies(layer, block, False)
            for n, width in NTILES:
                part = dots(layer, p, SEG_BLOCKS[s], n, width)
                acc[:, pl.ds(n, width)] = part if s == 0 else acc[:, pl.ds(n, width)] + part

        mate_copy(p).wait_recv()
        segment(0)
        if h == 1:
            @pl.when(layer == 0)
            def _():
                for block in range(NB):
                    if 2 * NB + block >= SLOTS:
                        w_copies(2, block, True)
        far_copy(p, 0).wait_recv()
        fwd_copy(p, 0).start()
        segment(1)
        far_copy(p, 1).wait_recv()
        fwd_copy(p, 1).start()
        fwd_copy(p, 0).wait_recv()
        segment(2)
        far_copy(p, 2).wait_recv()
        fwd_copy(p, 2).start()
        fwd_copy(p, 1).wait_recv()
        segment(3)
        far_copy(p, 3).wait_recv()
        fwd_copy(p, 3).start()
        fwd_copy(p, 2).wait_recv()
        segment(4)
        for c in range(NC):
            far_copy(p, c).wait_send()
        mate_copy(p).wait_send()
        for c in range(NC - 1):
            fwd_copy(p, c).wait_send()
        if h == 0:
            for block in SEG_BLOCKS[5]:
                w_copies(layer, block, False)
        fwd_copy(p, 3).wait_recv()

        def result(n, width):
            projected = acc[:, pl.ds(n, width)] + dots(layer, p, SEG_BLOCKS[5], n, width)
            shift = bias[0:1, pl.ds(n, width)]
            for other in range(1, LAYERS):
                shift = jnp.where(layer == other, bias[other:other + 1, pl.ds(n, width)], shift)
            shifted = projected + shift
            parts = []
            for i in range(width // TILE):
                t = n // TILE + i
                first = xb[h, OWN * NT + t].astype(jnp.float32)
                now = xb[p, OWN * NT + t].astype(jnp.float32)
                parts.append((first * shifted[:, i * TILE:(i + 1) * TILE] + now).astype(jnp.bfloat16))
            return parts

        @pl.when(layer < LAYERS - 1)
        def _():
            sent = 0
            for n, width in NTILES:
                for i, part in enumerate(result(n, width)):
                    xb[p + 2, OWN * NT + n // TILE + i] = part
                done = (n + width) // TILE
                while sent < NC and CHUNKS[sent][1] <= done - 2:
                    far_copy(p + 2, sent).start()
                    sent += 1
            while sent < NC:
                far_copy(p + 2, sent).start()
                sent += 1
            mate_copy(p + 2).start()

        @pl.when(layer == LAYERS - 1)
        def _():
            for n, width in NTILES:
                for i, part in enumerate(result(n, width)):
                    stage[h, :, pl.ds(n + i * TILE, TILE)] = part
            pltpu.make_async_copy(stage.at[h], out_hbm.at[pl.ds(h * HALF, HALF)], o_sem.at[h]).start()

        fwd_copy(p, NC - 1).wait_send()

    def layer_step(layer, carry):
        phase(layer, 0)
        phase(layer, 1)
        return carry

    lax.fori_loop(0, LAYERS, layer_step, 0)
    for h in range(2):
        pltpu.make_async_copy(stage.at[h], out_hbm.at[pl.ds(h * HALF, HALF)], o_sem.at[h]).wait()


def solution(mesh):
    def local_stack(x_loc, w_loc, b_loc):
        any_space = pl.BlockSpec(memory_space=pl.ANY)
        sem = pltpu.SemaphoreType.DMA
        return pl.pallas_call(
            kernel,
            out_shape=jax.ShapeDtypeStruct((ROWS, COLS), jnp.bfloat16),
            in_specs=[any_space] * 3,
            out_specs=any_space,
            scratch_shapes=[
                pltpu.VMEM((2 * LAYERS, 4 * NT, HALF, TILE), jnp.bfloat16),
                pltpu.VMEM((SLOTS, 2 * TILE, COLS), jnp.bfloat16),
                pltpu.VMEM((HALF, COLS), jnp.float32),
                pltpu.VMEM((LAYERS, COLS), jnp.float32),
                pltpu.VMEM((2, HALF, COLS), jnp.bfloat16),
                sem((SLOTS,)), sem((2,)), sem, sem((2,)),
                sem((2 * LAYERS, NC)), sem((2 * LAYERS, NC)),
                sem((2 * LAYERS, NC)), sem((2 * LAYERS, NC)),
                sem((2 * LAYERS,)), sem((2 * LAYERS,)),
            ],
            compiler_params=pltpu.CompilerParams(
                collective_id=0, has_side_effects=True, vmem_limit_bytes=66_000_000
            ),
            name="cross_stack",
        )(x_loc, w_loc, b_loc)

    return jax.shard_map(
        local_stack,
        mesh=mesh,
        in_specs=(P("dp", "tp"), P(None, None, "tp"), P(None, "tp")),
        out_specs=P("dp", "tp"),
        check_vma=False,
    )
```

```python
import functools

import jax
import jax.numpy as jnp
from jax import lax
from jax.experimental import pallas as pl
from jax.experimental.pallas import tpu as pltpu
from jax.sharding import PartitionSpec as P

MESH = pl.DeviceIdType.MESH
LAYERS, D, COLS, ROWS = 3, 6656, 1664, 128
HALF = ROWS // 2
TILE = 128
NT = COLS // TILE
OWN, MATE, FAR, FARMATE = range(4)
CHUNKS = ((0, 4), (4, 8), (8, 12), (12, 13))
NC = len(CHUNKS)


def tiles(role, chunk):
    return [(role, t) for t in range(*CHUNKS[chunk])]


SEGMENTS = [
    [(OWN, t) for t in range(NT)] + [(MATE, t) for t in range(NT)],
    tiles(FAR, 0),
    tiles(FAR, 1) + tiles(FARMATE, 0),
    tiles(FAR, 2) + tiles(FARMATE, 1),
    tiles(FARMATE, 2),
    tiles(FAR, 3) + tiles(FARMATE, 3),
]
SEQ = [t for s in SEGMENTS for t in s]
BLOCKS = [(SEQ[2 * i], SEQ[2 * i + 1]) for i in range(len(SEQ) // 2)]
NB = len(BLOCKS)
SEG_BLOCKS = []
_b = 0
for _s in SEGMENTS:
    SEG_BLOCKS.append(list(range(_b, _b + len(_s) // 2)))
    _b += len(_s) // 2
SLOTS = 65
AHEAD = ((3, 3, 3, 3, 2, 1), (3, 3, 2, 2, 1, 0))
NTILES = [(n, min(256, COLS - n)) for n in range(0, COLS, 256)]


def kernel(x_hbm, w_hbm, b_hbm, out_hbm, xb, wb, acc, bias, stage, w_sem, x_sem, b_sem, o_sem,
           far_send, far_recv, fwd_send, fwd_recv, mate_send, mate_recv):
    me = lax.axis_index("tp")
    mate = me + 1 - 2 * lax.rem(me, 2)
    far = lax.rem(me + 2, 4)
    farmate = lax.rem(mate + 2, 4)
    owners = (me, mate, far, farmate)

    def w_copies(layer, block, start):
        slot = lax.rem(layer * NB + block, SLOTS)
        (r0, t0), (r1, t1) = BLOCKS[block]
        if not start:
            pltpu.make_async_copy(w_hbm.at[0, pl.ds(0, 2 * TILE)], wb.at[slot], w_sem.at[slot]).wait()
        elif r0 == r1:
            row = pl.multiple_of(owners[r0] * COLS + t0 * TILE, TILE)
            pltpu.make_async_copy(w_hbm.at[layer, pl.ds(row, 2 * TILE)], wb.at[slot], w_sem.at[slot]).start()
        else:
            for i, (r, t) in enumerate(((r0, t0), (r1, t1))):
                row = pl.multiple_of(owners[r] * COLS + t * TILE, TILE)
                pltpu.make_async_copy(
                    w_hbm.at[layer, pl.ds(row, TILE)], wb.at[slot, pl.ds(i * TILE, TILE)], w_sem.at[slot]
                ).start()

    def far_copy(p, c):
        t0, t1 = CHUNKS[c]
        return pltpu.make_async_remote_copy(
            xb.at[p, pl.ds(OWN * NT + t0, t1 - t0)], xb.at[p, pl.ds(FAR * NT + t0, t1 - t0)],
            far_send.at[p, c], far_recv.at[p, c], device_id={"tp": far}, device_id_type=MESH)

    def fwd_copy(p, c):
        t0, t1 = CHUNKS[c]
        return pltpu.make_async_remote_copy(
            xb.at[p, pl.ds(FAR * NT + t0, t1 - t0)], xb.at[p, pl.ds(FARMATE * NT + t0, t1 - t0)],
            fwd_send.at[p, c], fwd_recv.at[p, c], device_id={"tp": mate}, device_id_type=MESH)

    def mate_copy(p):
        return pltpu.make_async_remote_copy(
            xb.at[p, pl.ds(OWN * NT, NT)], xb.at[p, pl.ds(MATE * NT, NT)],
            mate_send.at[p], mate_recv.at[p], device_id={"tp": mate}, device_id_type=MESH)

    for h in range(2):
        for t in range(NT):
            pltpu.make_async_copy(
                x_hbm.at[pl.ds(h * HALF, HALF), pl.ds(t * TILE, TILE)], xb.at[h, OWN * NT + t], x_sem.at[h]
            ).start()
    barrier = pltpu.get_barrier_semaphore()
    for other in (mate, far):
        pl.semaphore_signal(barrier, inc=1, device_id={"tp": other}, device_id_type=MESH)
    pltpu.make_async_copy(b_hbm, bias, b_sem).start()
    pl.semaphore_wait(barrier, 2)
    for h in range(2):
        pltpu.make_async_copy(xb.at[h, pl.ds(0, NT)], xb.at[h, pl.ds(0, NT)], x_sem.at[h]).wait()
        for c in range(NC):
            far_copy(h, c).start()
        mate_copy(h).start()
    for block in range(NB):
        w_copies(0, block, True)
    pltpu.make_async_copy(b_hbm, bias, b_sem).wait()

    def x_block(p, block):
        (r0, t0), (r1, t1) = BLOCKS[block]
        return jnp.concatenate([xb[p, r0 * NT + t0], xb[p, r1 * NT + t1]], axis=1)

    def dots(layer, p, blocks, n, width):
        total = None
        for block in blocks:
            slot = lax.rem(layer * NB + block, SLOTS)
            term = jnp.dot(x_block(p, block), wb[slot, :, pl.ds(n, width)], preferred_element_type=jnp.float32)
            total = term if total is None else total + term
        return total

    def phase(layer, h):
        p = 2 * layer + h

        def segment(s):
            if h == 0:
                for block in SEG_BLOCKS[s]:
                    w_copies(layer, block, False)
            for n, width in NTILES:
                part = dots(layer, p, SEG_BLOCKS[s], n, width)
                acc[:, pl.ds(n, width)] = part if s == 0 else acc[:, pl.ds(n, width)] + part
            ask(s)

        def ask(s):
            first = sum(AHEAD[0][:s]) if h == 0 else sum(AHEAD[0]) + sum(AHEAD[1][:s])

            @pl.when(layer < LAYERS - 1)
            def _():
                for block in range(first, first + AHEAD[h][s]):
                    w_copies(layer + 1, block, True)

        mate_copy(p).wait_recv()
        segment(0)
        far_copy(p, 0).wait_recv()
        fwd_copy(p, 0).start()
        segment(1)
        far_copy(p, 1).wait_recv()
        fwd_copy(p, 1).start()
        fwd_copy(p, 0).wait_recv()
        segment(2)
        far_copy(p, 2).wait_recv()
        fwd_copy(p, 2).start()
        fwd_copy(p, 1).wait_recv()
        segment(3)
        far_copy(p, 3).wait_recv()
        fwd_copy(p, 3).start()
        fwd_copy(p, 2).wait_recv()
        segment(4)
        for c in range(NC):
            far_copy(p, c).wait_send()
        mate_copy(p).wait_send()
        for c in range(NC - 1):
            fwd_copy(p, c).wait_send()
        if h == 0:
            for block in SEG_BLOCKS[5]:
                w_copies(layer, block, False)
        ask(5)
        fwd_copy(p, 3).wait_recv()

        def result(n, width):
            projected = acc[:, pl.ds(n, width)] + dots(layer, p, SEG_BLOCKS[5], n, width)
            shift = bias[0:1, pl.ds(n, width)]
            for other in range(1, LAYERS):
                shift = jnp.where(layer == other, bias[other:other + 1, pl.ds(n, width)], shift)
            shifted = projected + shift
            parts = []
            for i in range(width // TILE):
                t = n // TILE + i
                first = xb[h, OWN * NT + t].astype(jnp.float32)
                now = xb[p, OWN * NT + t].astype(jnp.float32)
                parts.append((first * shifted[:, i * TILE:(i + 1) * TILE] + now).astype(jnp.bfloat16))
            return parts

        @pl.when(layer < LAYERS - 1)
        def _():
            sent = 0
            for n, width in NTILES:
                for i, part in enumerate(result(n, width)):
                    xb[p + 2, OWN * NT + n // TILE + i] = part
                done = (n + width) // TILE
                while sent < NC and CHUNKS[sent][1] <= done - 2:
                    far_copy(p + 2, sent).start()
                    sent += 1
            while sent < NC:
                far_copy(p + 2, sent).start()
                sent += 1
            mate_copy(p + 2).start()

        @pl.when(layer == LAYERS - 1)
        def _():
            for n, width in NTILES:
                for i, part in enumerate(result(n, width)):
                    stage[h, :, pl.ds(n + i * TILE, TILE)] = part
            pltpu.make_async_copy(stage.at[h], out_hbm.at[pl.ds(h * HALF, HALF)], o_sem.at[h]).start()

        fwd_copy(p, NC - 1).wait_send()

    def layer_step(layer, carry):
        phase(layer, 0)
        phase(layer, 1)
        return carry

    lax.fori_loop(0, LAYERS, layer_step, 0)
    for h in range(2):
        pltpu.make_async_copy(stage.at[h], out_hbm.at[pl.ds(h * HALF, HALF)], o_sem.at[h]).wait()


def solution(mesh):
    def local_stack(x_loc, w_loc, b_loc):
        any_space = pl.BlockSpec(memory_space=pl.ANY)
        sem = pltpu.SemaphoreType.DMA
        return pl.pallas_call(
            kernel,
            out_shape=jax.ShapeDtypeStruct((ROWS, COLS), jnp.bfloat16),
            in_specs=[any_space] * 3,
            out_specs=any_space,
            scratch_shapes=[
                pltpu.VMEM((2 * LAYERS, 4 * NT, HALF, TILE), jnp.bfloat16),
                pltpu.VMEM((SLOTS, 2 * TILE, COLS), jnp.bfloat16),
                pltpu.VMEM((HALF, COLS), jnp.float32),
                pltpu.VMEM((LAYERS, COLS), jnp.float32),
                pltpu.VMEM((2, HALF, COLS), jnp.bfloat16),
                sem((SLOTS,)), sem((2,)), sem, sem((2,)),
                sem((2 * LAYERS, NC)), sem((2 * LAYERS, NC)),
                sem((2 * LAYERS, NC)), sem((2 * LAYERS, NC)),
                sem((2 * LAYERS,)), sem((2 * LAYERS,)),
            ],
            compiler_params=pltpu.CompilerParams(
                collective_id=0, has_side_effects=True, vmem_limit_bytes=66_000_000
            ),
            name="cross_stack",
        )(x_loc, w_loc, b_loc)

    return jax.shard_map(
        local_stack,
        mesh=mesh,
        in_specs=(P("dp", "tp"), P(None, None, "tp"), P(None, "tp")),
        out_specs=P("dp", "tp"),
        check_vma=False,
    )
```
